32 devices in a mesh: row: 8 (over y, x, core), col: 4 (over z).
Axes of the slice: x: 2, y: 2, z: 4, core: 2. Of those that a mesh axis runs over, the one named last changes fastest.
Arguments:
- covariance: bfloat16 [16384, 16384], P('row', 'col'), may hold values from -0.12 to 0.6, as said below
- estimate: bfloat16 [16384, 16384], P('row', 'col'), may hold values from -2.3 to 12, as said below
- dual_var: bfloat16 [16384, 16384], P('row', 'col'), may hold values from -1.7 to 1.7, as said below
- start_basis: float32 [16384, 128], P('row'), may hold values from -6 to 6
Outputs:
- next_estimate: float32 [16384, 16384], P('row', 'col')
- next_dual: bfloat16 [16384, 16384], P('row', 'col')
The draws below stay inside these ranges and needn't reach their ends.
Inputs may be any that keep to these rules, and one draw needn't show every extreme that they name: `covariance`: symmetric. `estimate`: symmetric. `dual_var`: symmetric.
All inputs are finite; a program needn't handle non-finite values.
Results may differ from the reference program's by a relative error of at most 0.001.
Values sent between devices are 32-bit elements; how exact they have to be, the bound alone decides.
A program may use at most 192 MiB of HBM per device.

```python
import jax
import jax.numpy as jnp
from jax import lax

P_SIZE = 16384
RANK = 128
ITERS = 1
NS_ITERS = 12
N_ROW = 8


def symmetric_part(key, spread):
    raw_draw = jax.random.truncated_normal(key, -4.0, 4.0, (P_SIZE, P_SIZE), jnp.float32)
    return (raw_draw + raw_draw.T) * (spread * 0.7071067811865476)


def on_diagonal():
    row_ids = lax.broadcasted_iota(jnp.int32, (P_SIZE, 1), 0)
    col_ids = lax.broadcasted_iota(jnp.int32, (1, P_SIZE), 1)
    return row_ids == col_ids


def draw_covariance(key, part):
    off_diag = symmetric_part(jax.random.fold_in(key, 11), 0.005)
    variances = jax.random.uniform(jax.random.fold_in(key, 12), (P_SIZE,), jnp.float32, 0.05, 0.15)
    matrix = jnp.where(on_diagonal(), variances[:, None], off_diag)
    return matrix.astype(jnp.bfloat16)


def draw_estimate(key, part):
    off_diag = symmetric_part(jax.random.fold_in(key, 21), 0.4)
    diagonal = jax.random.uniform(jax.random.fold_in(key, 22), (P_SIZE,), jnp.float32, 8.0, 12.0)
    return jnp.where(on_diagonal(), diagonal[:, None], off_diag).astype(jnp.bfloat16)


def draw_dual_var(key, part):
    return symmetric_part(jax.random.fold_in(key, 31), 0.3).astype(jnp.bfloat16)


def steps_of(stream_key, shape, split, least, top_value):
    def one(dim, blocks):
        steps = jax.random.uniform(jax.random.fold_in(jax.random.fold_in(stream_key, 6), dim), (blocks,), jnp.float32, least / len(split), top_value / len(split))
        return jnp.repeat(jnp.exp(steps), shape[dim] // blocks).reshape((-1,) + (1,) * (len(shape) - dim - 1))

    gain = one(*split[0])
    for cut in split[1:]:
        gain = gain * one(*cut)
    return gain


def bell_draw(stream_key, extent, scale, limit, cuts=(), kind=jnp.bfloat16):
    array = scale * jax.random.normal(stream_key, extent, jnp.float32)
    if cuts:
        array = array * steps_of(stream_key, extent, cuts, -0.22, 0.18)
    return jnp.clip(array, -limit, limit).astype(kind)


def setup_inputs(seed: int = 0) -> dict:
    keys = jax.random.split(jax.random.key(seed), 5)
    return {
        "covariance": draw_covariance(jax.random.fold_in(keys[4], 71), 0),
        "estimate": draw_estimate(jax.random.fold_in(keys[4], 71), 0),
        "dual_var": draw_dual_var(jax.random.fold_in(keys[4], 71), 0),
        "start_basis": bell_draw(keys[3], (P_SIZE, RANK), 1.0, 6.0, ((0, 8),), jnp.float32),
    }


penalty = 0.01
threshold = 0.2
base_level = 10.0
highest = lax.Precision.HIGHEST

def inner_product(left_side, right_side):
    return lax.dot_general(left_side.astype(jnp.float32), right_side.astype(jnp.float32), (((0,), (0,)), ((), ())), precision=highest, preferred_element_type=jnp.float32)

def normalize(mapped, gram_matrix):
    lower_factor = jnp.linalg.cholesky(gram_matrix)
    identity = jnp.eye(gram_matrix.shape[0], dtype=jnp.float32)
    inverse = lax.linalg.triangular_solve(lower_factor, identity, left_side=True, lower=True)
    return jnp.dot(mapped.astype(jnp.float32), inverse.T.astype(jnp.float32), precision=highest, preferred_element_type=jnp.float32)

def response_of(ritz_matrix):
    identity = jnp.eye(ritz_matrix.shape[0], dtype=jnp.float32)
    square = jnp.dot(ritz_matrix.astype(jnp.float32), ritz_matrix.astype(jnp.float32), precision=highest, preferred_element_type=jnp.float32) + 4.0 * penalty * identity
    frobenius = jnp.sqrt(jnp.sum(square * square))

    def newton(sweep_index, state_pair):
        iterate, partner = state_pair
        factor = 0.5 * (3.0 * identity - jnp.dot(partner.astype(jnp.float32), iterate.astype(jnp.float32), precision=highest, preferred_element_type=jnp.float32))
        return (jnp.dot(iterate.astype(jnp.float32), factor.astype(jnp.float32), precision=highest, preferred_element_type=jnp.float32), jnp.dot(factor.astype(jnp.float32), partner.astype(jnp.float32), precision=highest, preferred_element_type=jnp.float32))
    iterate, partner = lax.fori_loop(0, NS_ITERS, newton, (square / frobenius, identity))
    square_root = jnp.sqrt(frobenius) * iterate
    return (ritz_matrix + square_root) / (2.0 * penalty) - base_level * identity

def reference(covariance, estimate, dual_var, start_basis):
    shifted = penalty * (estimate.astype(jnp.float32) - dual_var.astype(jnp.float32)) - covariance.astype(jnp.float32)
    current = start_basis
    for sweep_index in range(ITERS):
        mapped = jnp.dot(shifted.astype(jnp.float32), current.astype(jnp.float32), precision=highest, preferred_element_type=jnp.float32)
        current = normalize(mapped, inner_product(mapped, mapped))
    product = jnp.dot(shifted.astype(jnp.float32), current.astype(jnp.float32), precision=highest, preferred_element_type=jnp.float32)
    raw_ritz = inner_product(current, product)
    ritz_matrix = 0.5 * (raw_ritz + raw_ritz.T)
    response = response_of(ritz_matrix)
    weighted = jnp.dot(current.astype(jnp.float32), response.astype(jnp.float32), precision=highest, preferred_element_type=jnp.float32)
    rows_block = P_SIZE // N_ROW

    def finish(block_index):
        row_start = block_index * rows_block
        left_rows = lax.dynamic_slice_in_dim(weighted, row_start, rows_block, 0)
        theta_tile = lax.dot_general(left_rows.astype(jnp.float32), current.astype(jnp.float32), (((1,), (1,)), ((), ())), precision=highest, preferred_element_type=jnp.float32)
        row_ids = row_start + lax.broadcasted_iota(jnp.int32, (rows_block, 1), 0)
        col_ids = lax.broadcasted_iota(jnp.int32, (1, P_SIZE), 1)
        theta_tile = theta_tile + jnp.where(row_ids == col_ids, base_level, 0.0)
        dual_rows = lax.dynamic_slice_in_dim(dual_var, row_start, rows_block, 0)
        mixture = theta_tile + dual_rows.astype(jnp.float32)
        clipped = jnp.clip(mixture, -threshold, threshold)
        return (mixture - clipped, clipped.astype(jnp.bfloat16))
    new_estimate, new_dual = lax.map(finish, jnp.arange(N_ROW, dtype=jnp.int32))
    return (new_estimate.reshape(P_SIZE, P_SIZE), new_dual.reshape(P_SIZE, P_SIZE))
```

```python
import functools

import jax
import jax.numpy as jnp
from jax import lax
from jax.experimental import pallas as pl
from jax.experimental.pallas import tpu as pltpu
from jax.sharding import PartitionSpec as P

NS_ITERS = 12


penalty = 0.01
threshold = 0.2
base_level = 10.0
highest = lax.Precision.HIGHEST


def from_root(value, axis, source):
    kept = jnp.where(lax.axis_index(axis) == source, value, 0).astype(value.dtype)
    return lax.psum(kept, axis)


def inner_product(left_side, right_side):
    return lax.dot_general(
        left_side,
        right_side,
        (((0,), (0,)), ((), ())),
        precision=highest,
        preferred_element_type=jnp.float32,
    )


def normalize(mapped, gram_matrix):
    lower_factor = jnp.linalg.cholesky(gram_matrix)
    identity = jnp.eye(gram_matrix.shape[0], dtype=jnp.float32)
    inverse = lax.linalg.triangular_solve(lower_factor, identity, left_side=True, lower=True)
    return jnp.dot(mapped, inverse.T, precision=highest, preferred_element_type=jnp.float32)


def response_of(ritz_matrix):
    identity = jnp.eye(ritz_matrix.shape[0], dtype=jnp.float32)
    square = (
        jnp.dot(ritz_matrix, ritz_matrix, precision=highest, preferred_element_type=jnp.float32)
        + 4.0 * penalty * identity
    )
    frobenius = jnp.sqrt(jnp.sum(square * square))

    def newton(sweep_index, state_pair):
        iterate, partner = state_pair
        factor = 0.5 * (
            3.0 * identity
            - jnp.dot(partner, iterate, precision=highest, preferred_element_type=jnp.float32)
        )
        return (
            jnp.dot(iterate, factor, precision=highest, preferred_element_type=jnp.float32),
            jnp.dot(factor, partner, precision=highest, preferred_element_type=jnp.float32),
        )

    iterate, partner = lax.fori_loop(0, NS_ITERS, newton, (square / frobenius, identity))
    square_root = jnp.sqrt(frobenius) * iterate
    return (ritz_matrix + square_root) / (2.0 * penalty) - base_level * identity


def column_basis(shifted, row_basis):
    partial_terms = lax.dot_general(
        shifted,
        row_basis,
        (((0,), (0,)), ((), ())),
        precision=highest,
        preferred_element_type=jnp.float32,
    )
    mapped = lax.psum(partial_terms, "row")
    gram_matrix = lax.psum(inner_product(mapped, mapped), "col")
    return normalize(mapped, gram_matrix)


def row_image(shifted, col_basis):
    local_terms = jnp.dot(shifted, col_basis, precision=highest, preferred_element_type=jnp.float32)
    return lax.psum(local_terms, "col")


def row_inner(left_side, right_side):
    return lax.psum(inner_product(left_side, right_side), "row")


def plain_body(covariance, estimate, dual_var, start_basis):
    shifted = penalty * (
        estimate.astype(jnp.float32) - dual_var.astype(jnp.float32)
    ) - covariance.astype(jnp.float32)
    rows_tile = shifted.shape[0]
    cols_tile = shifted.shape[1]
    row_basis = start_basis
    col_basis = column_basis(shifted, row_basis)
    blocks_per_column = lax.axis_size("row") // lax.axis_size("col")
    row_index = lax.axis_index("row")
    own_block = lax.dynamic_slice_in_dim(
        col_basis, row_index % blocks_per_column * rows_tile, rows_tile, 0
    )
    row_basis = from_root(own_block, "col", row_index // blocks_per_column)
    product = row_image(shifted, col_basis)
    raw_ritz = row_inner(row_basis, product)
    ritz_matrix = 0.5 * (raw_ritz + raw_ritz.T)
    response = response_of(ritz_matrix)
    weighted = jnp.dot(row_basis, response, precision=highest, preferred_element_type=jnp.float32)
    theta_tile = lax.dot_general(
        weighted,
        col_basis,
        (((1,), (1,)), ((), ())),
        precision=highest,
        preferred_element_type=jnp.float32,
    )
    row_ids = row_index * rows_tile + lax.broadcasted_iota(jnp.int32, (rows_tile, 1), 0)
    col_ids = lax.axis_index("col") * cols_tile + lax.broadcasted_iota(jnp.int32, (1, cols_tile), 1)
    theta_tile = theta_tile + jnp.where(row_ids == col_ids, base_level, 0.0)
    mixture = theta_tile + dual_var.astype(jnp.float32)
    clipped = jnp.clip(mixture, -threshold, threshold)
    return (mixture - clipped, clipped.astype(jnp.bfloat16))


MESH = pl.DeviceIdType.MESH
VMEM = pl.BlockSpec(memory_space=pltpu.VMEM)
VMEM_BYTES = 60 * 1024 * 1024


def high_dot(left_side, right_side, dims):
    return lax.dot_general(
        left_side, right_side, (dims, ((), ())), precision=highest, preferred_element_type=jnp.float32
    )


def split(value):
    upper = value.astype(jnp.bfloat16)
    return upper, (value - upper.astype(jnp.float32)).astype(jnp.bfloat16)


def fill_left(left_ref, index, basis_t):
    scaled_upper, scaled_lower = split(penalty * basis_t)
    upper, lower = split(basis_t)
    half = basis_t.shape[0]
    left_ref[0, index, :half] = scaled_upper
    left_ref[0, index, half:] = scaled_lower
    left_ref[1, index, :half] = -scaled_upper
    left_ref[1, index, half:] = -scaled_lower
    left_ref[2, index, :half] = -upper
    left_ref[2, index, half:] = -lower


def shifted_product(left_ref, tiles, acc_ref):
    blocks, depth = left_ref.shape[1], left_ref.shape[3]
    acc_ref[...] = jnp.zeros_like(acc_ref)

    def step(block, carry):
        rows = pl.ds(pl.multiple_of(block * depth, depth), depth)
        total = acc_ref[...]
        for which, tile in enumerate(tiles):
            total += jnp.dot(
                left_ref[which, block], tile[rows, :], preferred_element_type=jnp.float32
            )
        acc_ref[...] = total
        return carry

    lax.fori_loop(0, blocks, step, 0)
    half = acc_ref.shape[0] // 2
    return acc_ref[:half] + acc_ref[half:]


def image_kernel(est_ref, dual_ref, cov_ref, basis_ref, out_ref, left_ref, acc_ref):
    depth = left_ref.shape[3]

    @pl.when(pl.program_id(0) == 0)
    def _():
        for index in range(left_ref.shape[1]):
            fill_left(left_ref, index, basis_ref[index * depth : (index + 1) * depth, :].T)

    out_ref[0] = shifted_product(left_ref, (est_ref, dual_ref, cov_ref), acc_ref)


def moment_kernel(est_ref, dual_ref, cov_ref, rows_ref, cols_ref, out_ref, left_ref, acc_ref):
    step = pl.program_id(0)
    rank = rows_ref.shape[1]

    @pl.when(step == 0)
    def _():
        for index in range(left_ref.shape[1]):
            fill_left(left_ref, index, rows_ref[index])
        own = cols_ref[lax.axis_index("row")]
        out_ref[:rank] = high_dot(own, own, ((1,), (1,)))
        out_ref[rank:] = jnp.zeros((rank, rank), jnp.float32)

    image = shifted_product(left_ref, (est_ref, dual_ref, cov_ref), acc_ref)
    out_ref[rank:] += high_dot(image, cols_ref[step], ((1,), (1,)))


def local_call(kernel, matrices, extras, piece, depth, out_shape, out_spec):
    rows_tile, cols_tile = matrices[0].shape
    rank = 128
    tile_spec = pl.BlockSpec((rows_tile, piece), lambda step: (0, step))
    whole = [pl.BlockSpec(extra.shape, functools.partial(lambda n, step: (0,) * n, extra.ndim)) for extra in extras]
    rank = extras[0].shape[1]
    return pl.pallas_call(
        kernel,
        grid=(cols_tile // piece,),
        in_specs=[tile_spec] * 3 + whole,
        out_specs=out_spec,
        out_shape=out_shape,
        scratch_shapes=[
            pltpu.VMEM((3, rows_tile // depth, 2 * rank, depth), jnp.bfloat16),
            pltpu.VMEM((2 * rank, piece), jnp.float32),
        ],
        compiler_params=pltpu.CompilerParams(
            dimension_semantics=("arbitrary",), vmem_limit_bytes=VMEM_BYTES
        ),
    )(*matrices, *extras)


def spread_kernel(n_row, n_col, part_ref, mc_ref, mr_ref, near, other, zbuf, sems):
    row, col = lax.axis_index("row"), lax.axis_index("col")
    chips = n_row // 2
    chip, core = row // 2, row % 2
    sibling = chip * 2 + 1 - core
    ratio = n_row // n_col
    group = n_row // ratio

    barrier = pltpu.get_barrier_semaphore()

    def greet_row(t, carry):
        pl.semaphore_signal(barrier, inc=1, device_id=((row + t) % n_row, col), device_id_type=MESH)
        return carry

    def greet_col(t, carry):
        pl.semaphore_signal(barrier, inc=1, device_id=(row, (col + t) % n_col), device_id_type=MESH)
        return carry

    lax.fori_loop(1, n_row, greet_row, 0)
    lax.fori_loop(1, n_col, greet_col, 0)
    pl.semaphore_wait(barrier, n_row - 1 + n_col - 1)

    send1, recv1, send2, recv2, send3, recv3, send4, recv4, send5, recv5, send6, recv6 = sems

    def copy(src, dst, send, recv, target):
        return pltpu.make_async_remote_copy(
            src_ref=src, dst_ref=dst, send_sem=send, recv_sem=recv, device_id=target, device_id_type=MESH
        )

    first = []
    for t in range(chips):
        there = (chip + 1 + t) % chips
        first.append(
            copy(part_ref.at[2 * there + 1 - core], near.at[t], send1.at[t], recv1.at[t], (sibling, col))
        )
        first[-1].start()
    second = []
    for t in range(chips):
        there = (chip + 1 + t) % chips
        first[t].wait_recv()
        if t < chips - 1:
            near[t] = near[t] + part_ref[2 * there + core]
            second.append(
                copy(near.at[t], other.at[t], send2.at[t], recv2.at[t], (2 * there + core, col))
            )
            second[-1].start()
    total = near[chips - 1] + part_ref[row]
    for t in range(chips - 1):
        second[t].wait_recv()
        total += other[t]
    mc_ref[row] = total

    own = mc_ref.at[row]
    along = []
    for t in range(n_col - 1):
        along.append(copy(own, zbuf.at[t], send4.at[t], recv4.at[t], (row, (col + 1 + t) % n_col)))
        along[-1].start()
    plane = []
    for t in range(chips - 1):
        there = (chip + 1 + t) % chips
        plane.append(copy(own, own, send3.at[t], recv3.at[t], (2 * there + core, col)))
        plane[-1].start()
    pair = [copy(own, own, send5.at[0], recv5.at[0], (sibling, col))]
    pair[0].start()

    slot = row % group
    onward = []
    for t in range(n_col - 1):
        source = (col + n_col - 1 - t) % n_col
        target = source * ratio + row // group
        along[t].wait_recv()
        hop = copy(zbuf.at[t], mr_ref.at[slot], send6.at[t], recv6.at[slot], (target, col))

        @pl.when(target != row)
        def _():
            hop.start()

        @pl.when(target == row)
        def _():
            mr_ref[slot] = zbuf[t]

        onward.append((hop, target))

    for t in range(chips - 1):
        source = 2 * ((chip + chips - 1 - t) % chips) + core
        arrived = mc_ref.at[source]
        copy(own, arrived, send3.at[t], recv3.at[t], (row, col)).wait_recv()
        pair.append(copy(arrived, arrived, send5.at[t + 1], recv5.at[t + 1], (sibling, col)))
        pair[-1].start()
    for t in range(chips):
        source = 2 * ((chip + chips - t) % chips) + 1 - core
        copy(own, mc_ref.at[source], send5.at[t], recv5.at[t], (sibling, col)).wait_recv()

    @pl.when(row // ratio == col)
    def _():
        for k in range(group):
            mr_ref[k] = mc_ref[(row % ratio) * group + k]

    for k in range(group):
        @pl.when((row // ratio != col) & ((row % ratio) * group + k != row))
        def _():
            copy(zbuf.at[0], mr_ref.at[k], send6.at[0], recv6.at[k], (sibling, col)).wait_recv()

    for item in first + second + along + plane + pair:
        item.wait_send()
    for hop, target in onward:
        @pl.when(target != row)
        def _():
            hop.wait_send()


def spread(parts, n_row, n_col):
    rank, piece = parts.shape[1:]
    chips, ratio = n_row // 2, n_row // n_col
    group = n_row // ratio
    dma = pltpu.SemaphoreType.DMA

    def kernel(part_ref, mc_ref, mr_ref, near, other, zbuf, *sems):
        spread_kernel(n_row, n_col, part_ref, mc_ref, mr_ref, near, other, zbuf, sems)

    return pl.pallas_call(
        kernel,
        in_specs=[VMEM],
        out_specs=(VMEM, VMEM),
        out_shape=(
            jax.ShapeDtypeStruct((n_row, rank, piece), jnp.float32),
            jax.ShapeDtypeStruct((group, rank, piece), jnp.float32),
        ),
        scratch_shapes=[
            pltpu.VMEM((chips, rank, piece), jnp.float32),
            pltpu.VMEM((chips - 1, rank, piece), jnp.float32),
            pltpu.VMEM((n_col - 1, rank, piece), jnp.float32),
            dma((chips,)), dma((chips,)),
            dma((chips - 1,)), dma((chips - 1,)),
            dma((chips - 1,)), dma((chips - 1,)),
            dma((n_col - 1,)), dma((n_col - 1,)),
            dma((chips,)), dma((chips,)),
            dma((n_col - 1,)), dma((group,)),
        ],
        compiler_params=pltpu.CompilerParams(
            collective_id=0, has_side_effects=True, vmem_limit_bytes=VMEM_BYTES
        ),
    )(parts)


def total_kernel(n_row, n_col, term_ref, out_ref, terms, send1, recv1, send2, recv2):
    count = n_row * n_col
    row, col = lax.axis_index("row"), lax.axis_index("col")
    me = row * n_col + col
    barrier = pltpu.get_barrier_semaphore()

    def place(t):
        there = (me + t) % count
        return there, (there // n_col, there % n_col)

    def greet(t, carry):
        pl.semaphore_signal(barrier, inc=1, device_id=place(t)[1], device_id_type=MESH)
        return carry

    lax.fori_loop(1, count, greet, 0)
    pl.semaphore_wait(barrier, count - 1)

    def scatter(t):
        there, target = place(t)
        return pltpu.make_async_remote_copy(
            src_ref=term_ref.at[there], dst_ref=terms.at[t], send_sem=send1.at[t],
            recv_sem=recv1.at[t], device_id=target, device_id_type=MESH,
        )

    def gather(t, slot):
        return pltpu.make_async_remote_copy(
            src_ref=out_ref.at[me], dst_ref=out_ref.at[slot], send_sem=send2.at[t],
            recv_sem=recv2.at[t], device_id=place(t)[1], device_id_type=MESH,
        )

    def each(action):
        def step(t, carry):
            action(t)
            return carry

        lax.fori_loop(1, count, step, 0)

    each(lambda t: scatter(t).start())
    terms[0] = term_ref[me]
    each(lambda t: scatter(t).wait_recv())
    out_ref[me] = jnp.sum(terms[...], axis=0)
    each(lambda t: gather(t, me).start())
    each(lambda t: gather(t, (me + count - t) % count).wait_recv())
    each(lambda t: scatter(t).wait_send())
    each(lambda t: gather(t, me).wait_send())


def total(terms, n_row, n_col):
    count = n_row * n_col
    blocks = terms.reshape(count, terms.shape[0] // count, terms.shape[1])
    dma = pltpu.SemaphoreType.DMA
    summed = pl.pallas_call(
        functools.partial(total_kernel, n_row, n_col),
        in_specs=[VMEM],
        out_specs=VMEM,
        out_shape=jax.ShapeDtypeStruct(blocks.shape, jnp.float32),
        scratch_shapes=[pltpu.VMEM(blocks.shape, jnp.float32)] + [dma((count,))] * 4,
        compiler_params=pltpu.CompilerParams(collective_id=1, has_side_effects=True),
    )(blocks)
    return summed.reshape(terms.shape)


def weight_kernel(moment_ref, rows_ref, out_ref, inverse_ref, ritz_ref, iterate_ref, partner_ref):
    rank = rows_ref.shape[1]
    row_ids = lax.broadcasted_iota(jnp.int32, (rank, rank), 0)
    col_ids = lax.broadcasted_iota(jnp.int32, (rank, rank), 1)
    line_ids = lax.broadcasted_iota(jnp.int32, (1, rank), 1)
    identity = jnp.where(row_ids == col_ids, 1.0, 0.0)
    inverse = moment_ref[:rank]
    for k in range(rank):
        pivot = 1.0 / inverse[k : k + 1, k : k + 1]
        column = inverse[:, k : k + 1]
        line = jnp.where(line_ids == k, 1.0, inverse[k : k + 1, :]) * pivot
        inverse = jnp.where(
            row_ids == k, line, jnp.where(col_ids == k, 0.0, inverse) - column * line
        )
    inverse_ref[...] = inverse
    raw = moment_ref[rank:]
    iterate_ref[...] = 0.5 * (raw + raw.T)
    plain = ((1,), (0,))
    ritz_ref[...] = high_dot(inverse_ref[...], iterate_ref[...], plain)
    square = high_dot(ritz_ref[...], ritz_ref[...], plain) + 4.0 * penalty * identity
    frobenius = jnp.sqrt(jnp.sum(square * square.T, keepdims=True))
    iterate_ref[...] = square / frobenius
    partner_ref[...] = identity

    def newton(step, carry):
        iterate, partner = iterate_ref[...], partner_ref[...]
        factor = 0.5 * (3.0 * identity - high_dot(partner, iterate, plain))
        iterate_ref[...] = high_dot(iterate, factor, plain)
        partner_ref[...] = high_dot(factor, partner, plain)
        return carry

    lax.fori_loop(0, NS_ITERS, newton, 0)
    root = jnp.sqrt(frobenius) * iterate_ref[...]
    response = (ritz_ref[...] + root) / (2.0 * penalty) - base_level * identity
    partner_ref[...] = high_dot(response, inverse_ref[...], plain)
    piece = rows_ref.shape[2]
    for k in range(rows_ref.shape[0]):
        out_ref[k * piece : (k + 1) * piece, :] = high_dot(rows_ref[k].T, partner_ref[...], plain)


def finish_kernel(weighted_ref, cols_ref, dual_ref, est_ref, clip_ref, right_ref, low_ref):
    step = pl.program_id(0)
    count, rank, piece = cols_ref.shape
    depth = dual_ref.shape[0]

    @pl.when(step == 0)
    def _():
        for k in range(count):
            upper, lower = split(cols_ref[k])
            right_ref[k, :rank] = upper
            right_ref[k, rank:] = upper
            low_ref[k] = lower

    upper, lower = split(weighted_ref[...])
    both = jnp.concatenate([upper, lower], axis=1)
    n_grid = pl.num_programs(0)
    row_start = (lax.axis_index("row") * n_grid + step) * depth
    gap = (
        lax.broadcasted_iota(jnp.int32, (depth, piece), 1)
        - lax.broadcasted_iota(jnp.int32, (depth, piece), 0)
    )
    for k in range(count):
        where = slice(k * piece, (k + 1) * piece)
        col_start = lax.axis_index("col") * (count * piece) + k * piece
        theta = jnp.dot(both, right_ref[k], preferred_element_type=jnp.float32)
        theta += jnp.dot(upper, low_ref[k], preferred_element_type=jnp.float32)
        theta += jnp.where(gap == row_start - col_start, base_level, 0.0)
        mixture = theta + dual_ref[:, where].astype(jnp.float32)
        clipped = jnp.clip(mixture, -threshold, threshold)
        est_ref[:, where] = mixture - clipped
        clip_ref[:, where] = clipped.astype(jnp.bfloat16)


def finish(weighted, cols, dual_var):
    rows_tile, cols_tile = dual_var.shape
    count, rank, piece = cols.shape
    depth = min(256, rows_tile)
    wide = pl.BlockSpec((depth, cols_tile), lambda step: (step, 0))
    return pl.pallas_call(
        finish_kernel,
        grid=(rows_tile // depth,),
        in_specs=[
            pl.BlockSpec((depth, rank), lambda step: (step, 0)),
            pl.BlockSpec(cols.shape, lambda step: (0, 0, 0)),
            wide,
        ],
        out_specs=(wide, wide),
        out_shape=(
            jax.ShapeDtypeStruct(dual_var.shape, jnp.float32),
            jax.ShapeDtypeStruct(dual_var.shape, jnp.bfloat16),
        ),
        scratch_shapes=[
            pltpu.VMEM((count, 2 * rank, piece), jnp.bfloat16),
            pltpu.VMEM((count, rank, piece), jnp.bfloat16),
        ],
        compiler_params=pltpu.CompilerParams(
            dimension_semantics=("arbitrary",), vmem_limit_bytes=VMEM_BYTES
        ),
    )(weighted, cols, dual_var)


def fast_body(n_row, n_col, covariance, estimate, dual_var, start_basis):
    rows_tile, cols_tile = covariance.shape
    rank = start_basis.shape[1]
    piece = cols_tile // n_row
    matrices = (estimate, dual_var, covariance)
    parts = local_call(
        image_kernel, matrices, (start_basis,), piece, piece,
        jax.ShapeDtypeStruct((n_row, rank, piece), jnp.float32),
        pl.BlockSpec((1, rank, piece), lambda step: (step, 0, 0)),
    )
    cols, rows = spread(parts, n_row, n_col)
    moments = local_call(
        moment_kernel, matrices, (rows, cols), piece, piece,
        jax.ShapeDtypeStruct((2 * rank, rank), jnp.float32),
        pl.BlockSpec((2 * rank, rank), lambda step: (0, 0)),
    )
    moments = total(moments, n_row, n_col)
    weighted = pl.pallas_call(
        weight_kernel,
        in_specs=[VMEM, VMEM],
        out_specs=VMEM,
        out_shape=jax.ShapeDtypeStruct((rows_tile, rank), jnp.float32),
        scratch_shapes=[pltpu.VMEM((rank, rank), jnp.float32)] * 4,
        compiler_params=pltpu.CompilerParams(vmem_limit_bytes=VMEM_BYTES),
    )(moments, rows)
    return finish(weighted, cols, dual_var)


def body(covariance, estimate, dual_var, start_basis):
    n_row, n_col = lax.axis_size("row"), lax.axis_size("col")
    rows_tile, cols_tile = covariance.shape
    rank = start_basis.shape[1]
    piece = cols_tile // n_row
    fits = (
        n_row % 2 == 0
        and n_row % n_col == 0
        and cols_tile % n_row == 0
        and piece % 128 == 0
        and rows_tile % piece == 0
        and rank % 128 == 0
        and 2 * rank % (8 * n_row * n_col) == 0
    )
    if not fits:
        return plain_body(covariance, estimate, dual_var, start_basis)
    return fast_body(n_row, n_col, covariance, estimate, dual_var, start_basis)


def solution(mesh):
    return jax.shard_map(
        body,
        mesh=mesh,
        in_specs=(P("row", "col"), P("row", "col"), P("row", "col"), P("row", None)),
        out_specs=(P("row", "col"), P("row", "col")),
        check_vma=False,
    )
```

```python
import functools

import jax
import jax.numpy as jnp
from jax import lax
from jax.experimental import pallas as pl
from jax.experimental.pallas import tpu as pltpu
from jax.sharding import PartitionSpec as P

NS_ITERS = 12


penalty = 0.01
threshold = 0.2
base_level = 10.0
highest = lax.Precision.HIGHEST


def from_root(value, axis, source):
    kept = jnp.where(lax.axis_index(axis) == source, value, 0).astype(value.dtype)
    return lax.psum(kept, axis)


def inner_product(left_side, right_side):
    return lax.dot_general(
        left_side,
        right_side,
        (((0,), (0,)), ((), ())),
        precision=highest,
        preferred_element_type=jnp.float32,
    )


def normalize(mapped, gram_matrix):
    lower_factor = jnp.linalg.cholesky(gram_matrix)
    identity = jnp.eye(gram_matrix.shape[0], dtype=jnp.float32)
    inverse = lax.linalg.triangular_solve(lower_factor, identity, left_side=True, lower=True)
    return jnp.dot(mapped, inverse.T, precision=highest, preferred_element_type=jnp.float32)


def response_of(ritz_matrix):
    identity = jnp.eye(ritz_matrix.shape[0], dtype=jnp.float32)
    square = (
        jnp.dot(ritz_matrix, ritz_matrix, precision=highest, preferred_element_type=jnp.float32)
        + 4.0 * penalty * identity
    )
    frobenius = jnp.sqrt(jnp.sum(square * square))

    def newton(sweep_index, state_pair):
        iterate, partner = state_pair
        factor = 0.5 * (
            3.0 * identity
            - jnp.dot(partner, iterate, precision=highest, preferred_element_type=jnp.float32)
        )
        return (
            jnp.dot(iterate, factor, precision=highest, preferred_element_type=jnp.float32),
            jnp.dot(factor, partner, precision=highest, preferred_element_type=jnp.float32),
        )

    iterate, partner = lax.fori_loop(0, NS_ITERS, newton, (square / frobenius, identity))
    square_root = jnp.sqrt(frobenius) * iterate
    return (ritz_matrix + square_root) / (2.0 * penalty) - base_level * identity


def column_basis(shifted, row_basis):
    partial_terms = lax.dot_general(
        shifted,
        row_basis,
        (((0,), (0,)), ((), ())),
        precision=highest,
        preferred_element_type=jnp.float32,
    )
    mapped = lax.psum(partial_terms, "row")
    gram_matrix = lax.psum(inner_product(mapped, mapped), "col")
    return normalize(mapped, gram_matrix)


def row_image(shifted, col_basis):
    local_terms = jnp.dot(shifted, col_basis, precision=highest, preferred_element_type=jnp.float32)
    return lax.psum(local_terms, "col")


def row_inner(left_side, right_side):
    return lax.psum(inner_product(left_side, right_side), "row")


def plain_body(covariance, estimate, dual_var, start_basis):
    shifted = penalty * (
        estimate.astype(jnp.float32) - dual_var.astype(jnp.float32)
    ) - covariance.astype(jnp.float32)
    rows_tile = shifted.shape[0]
    cols_tile = shifted.shape[1]
    row_basis = start_basis
    col_basis = column_basis(shifted, row_basis)
    blocks_per_column = lax.axis_size("row") // lax.axis_size("col")
    row_index = lax.axis_index("row")
    own_block = lax.dynamic_slice_in_dim(
        col_basis, row_index % blocks_per_column * rows_tile, rows_tile, 0
    )
    row_basis = from_root(own_block, "col", row_index // blocks_per_column)
    product = row_image(shifted, col_basis)
    raw_ritz = row_inner(row_basis, product)
    ritz_matrix = 0.5 * (raw_ritz + raw_ritz.T)
    response = response_of(ritz_matrix)
    weighted = jnp.dot(row_basis, response, precision=highest, preferred_element_type=jnp.float32)
    theta_tile = lax.dot_general(
        weighted,
        col_basis,
        (((1,), (1,)), ((), ())),
        precision=highest,
        preferred_element_type=jnp.float32,
    )
    row_ids = row_index * rows_tile + lax.broadcasted_iota(jnp.int32, (rows_tile, 1), 0)
    col_ids = lax.axis_index("col") * cols_tile + lax.broadcasted_iota(jnp.int32, (1, cols_tile), 1)
    theta_tile = theta_tile + jnp.where(row_ids == col_ids, base_level, 0.0)
    mixture = theta_tile + dual_var.astype(jnp.float32)
    clipped = jnp.clip(mixture, -threshold, threshold)
    return (mixture - clipped, clipped.astype(jnp.bfloat16))


MESH = pl.DeviceIdType.MESH
VMEM = pl.BlockSpec(memory_space=pltpu.VMEM)
VMEM_BYTES = 60 * 1024 * 1024


def high_dot(left_side, right_side, dims):
    return lax.dot_general(
        left_side, right_side, (dims, ((), ())), precision=highest, preferred_element_type=jnp.float32
    )


def split(value):
    upper = value.astype(jnp.bfloat16)
    return upper, (value - upper.astype(jnp.float32)).astype(jnp.bfloat16)


def image_kernel(est_ref, dual_ref, cov_ref, basis_ref, out_ref, left_ref, acc_ref):
    blocks, both, depth = left_ref.shape
    half = both // 2

    @pl.when(pl.program_id(0) == 0)
    def _():
        for index in range(blocks):
            upper, lower = split(basis_ref[index * depth : (index + 1) * depth, :].T)
            left_ref[index, :half] = upper
            left_ref[index, half:] = lower

    acc_ref[...] = jnp.zeros_like(acc_ref)

    def step(block, carry):
        rows = pl.ds(pl.multiple_of(block * depth, depth), depth)
        shifted = penalty * (
            est_ref[rows, :].astype(jnp.float32) - dual_ref[rows, :].astype(jnp.float32)
        ) - cov_ref[rows, :].astype(jnp.float32)
        upper, lower = split(shifted)
        acc_ref[...] += jnp.dot(left_ref[block], upper, preferred_element_type=jnp.float32)
        acc_ref[:half] += jnp.dot(left_ref[block, :half], lower, preferred_element_type=jnp.float32)
        return carry

    lax.fori_loop(0, blocks, step, 0)
    out_ref[0] = acc_ref[:half] + acc_ref[half:]


def image_parts(matrices, start_basis, piece):
    rows_tile, cols_tile = matrices[0].shape
    rank = start_basis.shape[1]
    depth = min(256, rows_tile)
    return pl.pallas_call(
        image_kernel,
        grid=(cols_tile // piece,),
        in_specs=[pl.BlockSpec((rows_tile, piece), lambda step: (0, step))] * 3
        + [pl.BlockSpec(start_basis.shape, lambda step: (0, 0))],
        out_specs=pl.BlockSpec((1, rank, piece), lambda step: (step, 0, 0)),
        out_shape=jax.ShapeDtypeStruct((cols_tile // piece, rank, piece), jnp.float32),
        scratch_shapes=[
            pltpu.VMEM((rows_tile // depth, 2 * rank, depth), jnp.bfloat16),
            pltpu.VMEM((2 * rank, piece), jnp.float32),
        ],
        compiler_params=pltpu.CompilerParams(
            dimension_semantics=("arbitrary",), vmem_limit_bytes=VMEM_BYTES
        ),
    )(*matrices, start_basis)


def moment_kernel(est_ref, dual_ref, cov_ref, rows_ref, cols_ref, out_ref, right_ref):
    count, rank, piece = cols_ref.shape

    @pl.when(pl.program_id(0) == 0)
    def _():
        for k in range(count):
            flat = cols_ref[k].T
            scaled_upper, scaled_lower = split(penalty * flat)
            upper, lower = split(flat)
            right_ref[0, k, :, :rank] = scaled_upper
            right_ref[0, k, :, rank:] = scaled_lower
            right_ref[1, k, :, :rank] = -scaled_upper
            right_ref[1, k, :, rank:] = -scaled_lower
            right_ref[2, k, :, :rank] = -upper
            right_ref[2, k, :, rank:] = -lower
        own = cols_ref[lax.axis_index("row")]
        out_ref[:rank] = high_dot(own, own, ((1,), (1,)))
        out_ref[rank:] = jnp.zeros((rank, rank), jnp.float32)

    image = jnp.zeros((est_ref.shape[0], 2 * rank), jnp.float32)
    for k in range(count):
        where = slice(k * piece, (k + 1) * piece)
        for which, tile in enumerate((est_ref, dual_ref, cov_ref)):
            image += jnp.dot(tile[:, where], right_ref[which, k], preferred_element_type=jnp.float32)
    out_ref[rank:] += high_dot(rows_ref[0], image[:, :rank] + image[:, rank:], ((1,), (0,)))


def moment_terms(matrices, rows, cols):
    rows_tile, cols_tile = matrices[0].shape
    count, rank, piece = cols.shape
    depth = min(256, piece)
    per = piece // depth
    return pl.pallas_call(
        moment_kernel,
        grid=(rows_tile // depth,),
        in_specs=[pl.BlockSpec((depth, cols_tile), lambda step: (step, 0))] * 3
        + [
            pl.BlockSpec((1, rank, depth), lambda step: (step // per, 0, step % per)),
            pl.BlockSpec(cols.shape, lambda step: (0, 0, 0)),
        ],
        out_specs=pl.BlockSpec((2 * rank, rank), lambda step: (0, 0)),
        out_shape=jax.ShapeDtypeStruct((2 * rank, rank), jnp.float32),
        scratch_shapes=[pltpu.VMEM((3, count, piece, 2 * rank), jnp.bfloat16)],
        compiler_params=pltpu.CompilerParams(
            dimension_semantics=("arbitrary",), vmem_limit_bytes=VMEM_BYTES
        ),
    )(*matrices, rows, cols)


def spread_kernel(n_row, n_col, part_ref, mc_ref, mr_ref, near, other, zbuf, sems):
    row, col = lax.axis_index("row"), lax.axis_index("col")
    chips = n_row // 2
    chip, core = row // 2, row % 2
    sibling = chip * 2 + 1 - core
    ratio = n_row // n_col
    group = n_row // ratio

    barrier = pltpu.get_barrier_semaphore()

    def greet_row(t, carry):
        pl.semaphore_signal(barrier, inc=1, device_id=((row + t) % n_row, col), device_id_type=MESH)
        return carry

    def greet_col(t, carry):
        pl.semaphore_signal(barrier, inc=1, device_id=(row, (col + t) % n_col), device_id_type=MESH)
        return carry

    lax.fori_loop(1, n_row, greet_row, 0)
    lax.fori_loop(1, n_col, greet_col, 0)
    pl.semaphore_wait(barrier, n_row - 1 + n_col - 1)

    send1, recv1, send2, recv2, send3, recv3, send4, recv4, send5, recv5, send6, recv6 = sems

    def copy(src, dst, send, recv, target):
        return pltpu.make_async_remote_copy(
            src_ref=src, dst_ref=dst, send_sem=send, recv_sem=recv, device_id=target, device_id_type=MESH
        )

    first = []
    for t in range(chips):
        there = (chip + 1 + t) % chips
        first.append(
            copy(part_ref.at[2 * there + 1 - core], near.at[t], send1.at[t], recv1.at[t], (sibling, col))
        )
        first[-1].start()
    second = []
    for t in range(chips):
        there = (chip + 1 + t) % chips
        first[t].wait_recv()
        if t < chips - 1:
            near[t] = near[t] + part_ref[2 * there + core]
            second.append(
                copy(near.at[t], other.at[t], send2.at[t], recv2.at[t], (2 * there + core, col))
            )
            second[-1].start()
    total = near[chips - 1] + part_ref[row]
    for t in range(chips - 1):
        second[t].wait_recv()
        total += other[t]
    mc_ref[row] = total

    own = mc_ref.at[row]
    along = []
    for t in range(n_col - 1):
        along.append(copy(own, zbuf.at[t], send4.at[t], recv4.at[t], (row, (col + 1 + t) % n_col)))
        along[-1].start()
    plane = []
    for t in range(chips - 1):
        there = (chip + 1 + t) % chips
        plane.append(copy(own, own, send3.at[t], recv3.at[t], (2 * there + core, col)))
        plane[-1].start()
    pair = [copy(own, own, send5.at[0], recv5.at[0], (sibling, col))]
    pair[0].start()

    slot = row % group
    onward = []
    for t in range(n_col - 1):
        source = (col + n_col - 1 - t) % n_col
        target = source * ratio + row // group
        along[t].wait_recv()
        hop = copy(zbuf.at[t], mr_ref.at[slot], send6.at[t], recv6.at[slot], (target, col))

        @pl.when(target != row)
        def _():
            hop.start()

        @pl.when(target == row)
        def _():
            mr_ref[slot] = zbuf[t]

        onward.append((hop, target))

    for t in range(chips - 1):
        source = 2 * ((chip + chips - 1 - t) % chips) + core
        arrived = mc_ref.at[source]
        copy(own, arrived, send3.at[t], recv3.at[t], (row, col)).wait_recv()
        pair.append(copy(arrived, arrived, send5.at[t + 1], recv5.at[t + 1], (sibling, col)))
        pair[-1].start()
    for t in range(chips):
        source = 2 * ((chip + chips - t) % chips) + 1 - core
        copy(own, mc_ref.at[source], send5.at[t], recv5.at[t], (sibling, col)).wait_recv()

    @pl.when(row // ratio == col)
    def _():
        for k in range(group):
            mr_ref[k] = mc_ref[(row % ratio) * group + k]

    for k in range(group):
        @pl.when((row // ratio != col) & ((row % ratio) * group + k != row))
        def _():
            copy(zbuf.at[0], mr_ref.at[k], send6.at[0], recv6.at[k], (sibling, col)).wait_recv()

    for item in first + second + along + plane + pair:
        item.wait_send()
    for hop, target in onward:
        @pl.when(target != row)
        def _():
            hop.wait_send()


def spread(parts, n_row, n_col):
    rank, piece = parts.shape[1:]
    chips, ratio = n_row // 2, n_row // n_col
    group = n_row // ratio
    dma = pltpu.SemaphoreType.DMA

    def kernel(part_ref, mc_ref, mr_ref, near, other, zbuf, *sems):
        spread_kernel(n_row, n_col, part_ref, mc_ref, mr_ref, near, other, zbuf, sems)

    return pl.pallas_call(
        kernel,
        in_specs=[VMEM],
        out_specs=(VMEM, VMEM),
        out_shape=(
            jax.ShapeDtypeStruct((n_row, rank, piece), jnp.float32),
            jax.ShapeDtypeStruct((group, rank, piece), jnp.float32),
        ),
        scratch_shapes=[
            pltpu.VMEM((chips, rank, piece), jnp.float32),
            pltpu.VMEM((chips - 1, rank, piece), jnp.float32),
            pltpu.VMEM((n_col - 1, rank, piece), jnp.float32),
            dma((chips,)), dma((chips,)),
            dma((chips - 1,)), dma((chips - 1,)),
            dma((chips - 1,)), dma((chips - 1,)),
            dma((n_col - 1,)), dma((n_col - 1,)),
            dma((chips,)), dma((chips,)),
            dma((n_col - 1,)), dma((group,)),
        ],
        compiler_params=pltpu.CompilerParams(
            collective_id=0, has_side_effects=True, vmem_limit_bytes=VMEM_BYTES
        ),
    )(parts)


def total_kernel(n_row, n_col, term_ref, out_ref, terms, part, planes, *sems):
    send1, recv1, send2, recv2, send3, recv3 = sems
    row, col = lax.axis_index("row"), lax.axis_index("col")
    barrier = pltpu.get_barrier_semaphore()

    def greet_row(t, carry):
        pl.semaphore_signal(barrier, inc=1, device_id=((row + t) % n_row, col), device_id_type=MESH)
        return carry

    def greet_col(t, carry):
        pl.semaphore_signal(barrier, inc=1, device_id=(row, (col + t) % n_col), device_id_type=MESH)
        return carry

    lax.fori_loop(1, n_row, greet_row, 0)
    lax.fori_loop(1, n_col, greet_col, 0)
    pl.semaphore_wait(barrier, n_row - 1 + n_col - 1)

    def copy(src, dst, send, recv, target):
        return pltpu.make_async_remote_copy(
            src_ref=src, dst_ref=dst, send_sem=send, recv_sem=recv, device_id=target, device_id_type=MESH
        )

    first = []
    for t in range(1, n_row):
        there = (row + t) % n_row
        first.append(copy(term_ref.at[there], terms.at[t], send1.at[t], recv1.at[t], (there, col)))
        first[-1].start()
    summed = term_ref[row]
    for t in range(1, n_row):
        first[t - 1].wait_recv()
        summed += terms[t]
    part[...] = summed
    second = []
    for t in range(1, n_col):
        there = (col + t) % n_col
        second.append(copy(part, planes.at[col], send2.at[t], recv2.at[col], (row, there)))
        second[-1].start()
    planes[col] = summed
    for t in range(1, n_col):
        source = (col + t) % n_col
        copy(part, planes.at[source], send2.at[t], recv2.at[source], (row, source)).wait_recv()
    out_ref[row] = jnp.sum(planes[...], axis=0)
    third = []
    for t in range(1, n_row):
        there = (row + t) % n_row
        third.append(copy(out_ref.at[row], out_ref.at[row], send3.at[t], recv3.at[t], (there, col)))
        third[-1].start()
    for t in range(1, n_row):
        source = (row + n_row - t) % n_row
        copy(out_ref.at[row], out_ref.at[source], send3.at[t], recv3.at[t], (source, col)).wait_recv()
    for item in first + second + third:
        item.wait_send()


def total(terms, n_row, n_col):
    blocks = terms.reshape(n_row, terms.shape[0] // n_row, terms.shape[1])
    block = blocks.shape[1:]
    dma = pltpu.SemaphoreType.DMA
    summed = pl.pallas_call(
        functools.partial(total_kernel, n_row, n_col),
        in_specs=[VMEM],
        out_specs=VMEM,
        out_shape=jax.ShapeDtypeStruct(blocks.shape, jnp.float32),
        scratch_shapes=[
            pltpu.VMEM(blocks.shape, jnp.float32),
            pltpu.VMEM(block, jnp.float32),
            pltpu.VMEM((n_col, *block), jnp.float32),
            dma((n_row,)), dma((n_row,)),
            dma((n_col,)), dma((n_col,)),
            dma((n_row,)), dma((n_row,)),
        ],
        compiler_params=pltpu.CompilerParams(collective_id=1, has_side_effects=True),
    )(blocks)
    return summed.reshape(terms.shape)


def weight_kernel(moment_ref, rows_ref, out_ref, inverse_ref, ritz_ref, iterate_ref, partner_ref):
    rank = rows_ref.shape[1]
    row_ids = lax.broadcasted_iota(jnp.int32, (rank, rank), 0)
    col_ids = lax.broadcasted_iota(jnp.int32, (rank, rank), 1)
    line_ids = lax.broadcasted_iota(jnp.int32, (1, rank), 1)
    identity = jnp.where(row_ids == col_ids, 1.0, 0.0)
    inverse = moment_ref[:rank]
    for k in range(rank):
        pivot = 1.0 / inverse[k : k + 1, k : k + 1]
        column = inverse[:, k : k + 1]
        line = jnp.where(line_ids == k, 1.0, inverse[k : k + 1, :]) * pivot
        inverse = jnp.where(
            row_ids == k, line, jnp.where(col_ids == k, 0.0, inverse) - column * line
        )
    inverse_ref[...] = inverse
    raw = moment_ref[rank:]
    iterate_ref[...] = 0.5 * (raw + raw.T)
    plain = ((1,), (0,))
    ritz_ref[...] = high_dot(inverse_ref[...], iterate_ref[...], plain)
    square = high_dot(ritz_ref[...], ritz_ref[...], plain) + 4.0 * penalty * identity
    frobenius = jnp.sqrt(jnp.sum(square * square.T, keepdims=True))
    iterate_ref[...] = square / frobenius
    partner_ref[...] = identity

    def newton(step, carry):
        iterate, partner = iterate_ref[...], partner_ref[...]
        factor = 0.5 * (3.0 * identity - high_dot(partner, iterate, plain))
        iterate_ref[...] = high_dot(iterate, factor, plain)
        partner_ref[...] = high_dot(factor, partner, plain)
        return carry

    lax.fori_loop(0, NS_ITERS, newton, 0)
    root = jnp.sqrt(frobenius) * iterate_ref[...]
    response = (ritz_ref[...] + root) / (2.0 * penalty) - base_level * identity
    partner_ref[...] = high_dot(response, inverse_ref[...], plain)
    piece = rows_ref.shape[2]
    for k in range(rows_ref.shape[0]):
        out_ref[k * piece : (k + 1) * piece, :] = high_dot(rows_ref[k].T, partner_ref[...], plain)


def finish_kernel(weighted_ref, cols_ref, dual_ref, est_ref, clip_ref, right_ref, low_ref):
    step = pl.program_id(0)
    count, rank, piece = cols_ref.shape
    depth = dual_ref.shape[0]

    @pl.when(step == 0)
    def _():
        for k in range(count):
            upper, lower = split(cols_ref[k])
            right_ref[k, :rank] = upper
            right_ref[k, rank:] = upper
            low_ref[k] = lower

    upper, lower = split(weighted_ref[...])
    both = jnp.concatenate([upper, lower], axis=1)
    n_grid = pl.num_programs(0)
    row_start = (lax.axis_index("row") * n_grid + step) * depth
    gap = (
        lax.broadcasted_iota(jnp.int32, (depth, piece), 1)
        - lax.broadcasted_iota(jnp.int32, (depth, piece), 0)
    )
    for k in range(count):
        where = slice(k * piece, (k + 1) * piece)
        col_start = lax.axis_index("col") * (count * piece) + k * piece
        theta = jnp.dot(both, right_ref[k], preferred_element_type=jnp.float32)
        theta += jnp.dot(upper, low_ref[k], preferred_element_type=jnp.float32)
        theta += jnp.where(gap == row_start - col_start, base_level, 0.0)
        mixture = theta + dual_ref[:, where].astype(jnp.float32)
        clipped = jnp.clip(mixture, -threshold, threshold)
        est_ref[:, where] = mixture - clipped
        clip_ref[:, where] = clipped.astype(jnp.bfloat16)


def finish(weighted, cols, dual_var):
    rows_tile, cols_tile = dual_var.shape
    count, rank, piece = cols.shape
    depth = min(512, rows_tile)
    wide = pl.BlockSpec((depth, cols_tile), lambda step: (step, 0))
    return pl.pallas_call(
        finish_kernel,
        grid=(rows_tile // depth,),
        in_specs=[
            pl.BlockSpec((depth, rank), lambda step: (step, 0)),
            pl.BlockSpec(cols.shape, lambda step: (0, 0, 0)),
            wide,
        ],
        out_specs=(wide, wide),
        out_shape=(
            jax.ShapeDtypeStruct(dual_var.shape, jnp.float32),
            jax.ShapeDtypeStruct(dual_var.shape, jnp.bfloat16),
        ),
        scratch_shapes=[
            pltpu.VMEM((count, 2 * rank, piece), jnp.bfloat16),
            pltpu.VMEM((count, rank, piece), jnp.bfloat16),
        ],
        compiler_params=pltpu.CompilerParams(
            dimension_semantics=("arbitrary",), vmem_limit_bytes=VMEM_BYTES
        ),
    )(weighted, cols, dual_var)


def fast_body(n_row, n_col, covariance, estimate, dual_var, start_basis):
    rows_tile, cols_tile = covariance.shape
    rank = start_basis.shape[1]
    piece = cols_tile // n_row
    matrices = (estimate, dual_var, covariance)
    parts = image_parts(matrices, start_basis, piece)
    cols, rows = spread(parts, n_row, n_col)
    moments = moment_terms(matrices, rows, cols)
    moments = total(moments, n_row, n_col)
    weighted = pl.pallas_call(
        weight_kernel,
        in_specs=[VMEM, VMEM],
        out_specs=VMEM,
        out_shape=jax.ShapeDtypeStruct((rows_tile, rank), jnp.float32),
        scratch_shapes=[pltpu.VMEM((rank, rank), jnp.float32)] * 4,
        compiler_params=pltpu.CompilerParams(vmem_limit_bytes=VMEM_BYTES),
    )(moments, rows)
    return finish(weighted, cols, dual_var)


def body(covariance, estimate, dual_var, start_basis):
    n_row, n_col = lax.axis_size("row"), lax.axis_size("col")
    rows_tile, cols_tile = covariance.shape
    rank = start_basis.shape[1]
    piece = cols_tile // n_row
    fits = (
        n_row % 2 == 0
        and n_row % n_col == 0
        and cols_tile % n_row == 0
        and piece % 128 == 0
        and rows_tile % piece == 0
        and rank % 128 == 0
        and 2 * rank % (8 * n_row) == 0
    )
    if not fits:
        return plain_body(covariance, estimate, dual_var, start_basis)
    return fast_body(n_row, n_col, covariance, estimate, dual_var, start_basis)


def solution(mesh):
    return jax.shard_map(
        body,
        mesh=mesh,
        in_specs=(P("row", "col"), P("row", "col"), P("row", "col"), P("row", None)),
        out_specs=(P("row", "col"), P("row", "col")),
        check_vma=False,
    )
```
